32 devices in a mesh: gx: 8 (over z, x), gy: 4 (over y, core).
Axes of the slice: x: 2, y: 2, z: 4, core: 2. Of those that a mesh axis runs over, the one named last changes fastest.
Arguments:
- mode_fields: float32 [32, 512, 1024], P(None, 'gx', 'gy'), may hold values from -60 to 60, as said below
- conductance: float32 [512, 1024], P('gx', 'gy'), may hold values from 0.5 to 2
- potential: float32 [512, 1024], P('gx', 'gy'), may hold values from 0.25 to 4
Outputs:
- basis_field: float32 [128, 512, 1024], P(None, 'gx', 'gy')
- scaled_factor: float32 [128, 128], replicated
The draws below stay inside these ranges and needn't reach their ends.
Inputs may be any that keep to these rules, and one draw needn't show every extreme that they name: `mode_fields`: Real-valued mode amplitudes.
All inputs are finite; a program needn't handle non-finite values.
Results may differ from the reference program's by a relative error of at most 0.0003.
Values sent between devices are 32-bit elements; how exact they have to be, the bound alone decides.
A program may use at most 64 MiB of HBM per device.

```python
import math
import jax
import jax.numpy as jnp
from jax import lax

K = 32
C = 128
CX = 64
NX = 512
NY = 1024


def draw_mode_fields(key, part):
    key_scale, key_noise = jax.random.split(key, 2)
    col_scale = 10.0 ** jax.random.uniform(key_scale, (K, 1, 1), jnp.float32, -0.5, 0.5)
    row_pos = jnp.arange(NX, dtype=jnp.float32) / max(NX - 1, 1)
    row_scale = (10.0 ** (row_pos - 0.5))[None, :, None]
    noise = jax.random.truncated_normal(key_noise, -6.0, 6.0, (K, NX, NY), jnp.float32)
    return (col_scale * row_scale * noise).astype(jnp.float32)


def levels(own_key, dims, cuts, smallest, largest):
    def one(axis_at, shards_of):
        draws = jax.random.uniform(jax.random.fold_in(jax.random.fold_in(own_key, 6), axis_at), (shards_of,), jnp.float32, smallest / len(cuts), largest / len(cuts))
        return jnp.repeat(jnp.exp(draws), dims[axis_at] // shards_of).reshape((-1,) + (1,) * (len(dims) - axis_at - 1))

    loudness = one(*cuts[0])
    for cut in cuts[1:]:
        loudness = loudness * one(*cut)
    return loudness


def setup_inputs(seed: int = 0) -> dict:
    key_list = jax.random.split(jax.random.key(seed), 4)
    mode_fields = draw_mode_fields(jax.random.fold_in(key_list[3], 71), 0)
    conductance = jnp.clip(jnp.exp(math.log(2.0) - 1.3862944 * jax.random.uniform(key_list[1], (NX, NY), jnp.float32) ** levels(key_list[1], (NX, NY), ((0, 8), (1, 4)), -0.2, 0.2)), 0.5, 2.0)
    potential = jnp.clip(jnp.exp(math.log(4.0) - 2.7725887 * jax.random.uniform(key_list[2], (NX, NY), jnp.float32) ** levels(key_list[2], (NX, NY), ((0, 8), (1, 4)), -0.2, 0.2)), 0.25, 4.0)
    return {"mode_fields": mode_fields, "conductance": conductance, "potential": potential}


def build_columns(fields, conduct, potential):
    center = fields[:, 1:-1, 1:-1]
    k_mid = conduct[1:-1, 1:-1]
    x_plus = 0.5 * (k_mid + conduct[2:, 1:-1])
    x_minus = 0.5 * (k_mid + conduct[:-2, 1:-1])
    y_plus = 0.5 * (k_mid + conduct[1:-1, 2:])
    y_minus = 0.5 * (k_mid + conduct[1:-1, :-2])
    along_x = x_plus * (center - fields[:, 2:, 1:-1]) + x_minus * (center - fields[:, :-2, 1:-1])
    along_y = y_plus * (center - fields[:, 1:-1, 2:]) + y_minus * (center - fields[:, 1:-1, :-2])
    react = potential * center
    stacked = jnp.concatenate([center, along_x, along_y, react], 0)
    return stacked.reshape(stacked.shape[0], -1)

def reference(mode_fields, conductance, potential):
    pad_u = jnp.pad(mode_fields, ((0, 0), (1, 1), (1, 1)))
    pad_k = jnp.pad(conductance, 1)
    strips = NX // CX
    cell_count = float(NX * NY)

    def strip_columns(index):
        start = (index * CX).astype(jnp.int32)
        fields = lax.dynamic_slice_in_dim(pad_u, start, CX + 2, 1)
        conduct = lax.dynamic_slice_in_dim(pad_k, start, CX + 2, 0)
        react = lax.dynamic_slice_in_dim(potential, start, CX, 0)
        return build_columns(fields, conduct, react)

    def add_gram(carry, index):
        matrix = strip_columns(index)
        return (carry + jnp.dot(matrix, matrix.T, precision=lax.Precision.HIGHEST), None)
    indices = jnp.arange(strips, dtype=jnp.int32)
    gram_total, _ = lax.scan(add_gram, jnp.zeros((C, C), jnp.float32), indices)
    lower_tri = jnp.linalg.cholesky(gram_total / cell_count)

    def solve_strip(index):
        solved = jax.scipy.linalg.solve_triangular(lower_tri, strip_columns(index), lower=True)
        return solved.reshape(C, CX, NY)
    blocks = lax.map(solve_strip, indices)
    basis_field = blocks.transpose(1, 0, 2, 3).reshape(C, NX, NY)
    return (basis_field, lower_tri.T)
```

```python
import functools

import jax
import jax.numpy as jnp
from jax import lax
from jax.experimental import pallas as pl
from jax.experimental.pallas import tpu as pltpu
from jax.sharding import PartitionSpec as P

MESH = pl.DeviceIdType.MESH
F32 = jnp.float32
BF16 = jnp.bfloat16


def split(value):
    high = value.astype(BF16)
    return high, (value - high.astype(F32)).astype(BF16)


def gram_kernel(
    nx, ny, u_hbm, k_ref, p_ref, m_ref, g_ref,
    flat, load, wide, edge, halo, acc, part, piece, ring, full,
    halo_send, halo_recv, rs_send, rs_recv, all_send, all_recv, ag_send, ag_recv,
):
    rows, cols = k_ref.shape
    modes = u_hbm.shape[0] // rows
    tiles = cols // 128
    columns = 4 * modes
    share = columns // ny
    px, py = lax.axis_index("gx"), lax.axis_index("gy")

    loads = [
        pltpu.make_async_copy(u_hbm.at[:, pl.ds(t * 128, 128)], flat.at[t], load.at[t]) for t in range(tiles)
    ]
    for copy in loads:
        copy.start()
    barrier = pltpu.get_barrier_semaphore()
    for d in range(1, nx):
        pl.semaphore_signal(barrier, inc=1, device_id={"gx": lax.rem(px + d, nx)}, device_id_type=MESH)
    for d in range(1, ny):
        pl.semaphore_signal(barrier, inc=1, device_id={"gy": lax.rem(py + d, ny)}, device_id_type=MESH)

    lanes = lax.broadcasted_iota(jnp.int32, (modes + 8, 128), 1)

    def spread(i, carry):
        first, last = carry
        row = jnp.concatenate(
            [jnp.concatenate([flat[t, pl.ds(i, modes, stride=rows), :] for t in range(tiles)], 1),
             jnp.broadcast_to(k_ref[pl.ds(i, 1), :], (8, cols))], 0
        )
        wide[i + 1] = row
        first = jnp.where(lanes == i, pltpu.roll(row[:, :128], i, 1), first)
        last = jnp.where(lanes == i, pltpu.roll(row[:, cols - 128:], lax.rem(i + 1, 128), 1), last)
        return first, last

    for copy in loads:
        copy.wait()
    zero = jnp.zeros((modes + 8, 128), F32)
    first, last = lax.fori_loop(0, rows, spread, (zero, zero), unroll=4)
    edge[0] = first
    edge[1] = last

    pl.semaphore_wait(barrier, nx + ny - 2)
    right, left = lax.rem(py + 1, ny), lax.rem(py + ny - 1, ny)
    down, up = lax.rem(px + 1, nx), lax.rem(px + nx - 1, nx)
    moves = (
        (edge.at[1], halo.at[0], {"gy": right}),
        (edge.at[0], halo.at[1], {"gy": left}),
        (wide.at[rows], wide.at[0], {"gx": down}),
        (wide.at[1], wide.at[rows + 1], {"gx": up}),
    )
    copies = [
        pltpu.make_async_remote_copy(
            src_ref=src, dst_ref=dst, send_sem=halo_send.at[n], recv_sem=halo_recv.at[n],
            device_id=device, device_id_type=MESH,
        )
        for n, (src, dst, device) in enumerate(moves)
    ]
    for copy in copies:
        copy.start()
    for copy in copies:
        copy.wait()
    wide[0] = jnp.where(px > 0, wide[0], 0.0)
    wide[rows + 1] = jnp.where(px < nx - 1, wide[rows + 1], 0.0)
    halo[0] = jnp.where(py > 0, halo[0], 0.0)
    halo[1] = jnp.where(py < ny - 1, halo[1], 0.0)

    group = 4
    span = lax.broadcasted_iota(jnp.int32, (modes + 8, cols), 1)
    acc[...] = jnp.zeros_like(acc)

    def build(g, _):
        for s in range(group):
            i = g * group + s
            row = wide[i + 1]
            center, k_mid = row[:modes], row[modes:modes + 1]
            after, before = wide[i + 2], wide[i]
            pad = jnp.zeros((modes + 8, cols - 128), F32)
            left_edge = jnp.concatenate([pltpu.roll(halo[0], lax.rem(128 - i, 128), 1), pad], 1)
            right_edge = jnp.concatenate([pad, pltpu.roll(halo[1], 127 - i, 1)], 1)
            to_left = jnp.where(span == 0, left_edge, pltpu.roll(row, 1, 1))
            to_right = jnp.where(span == cols - 1, right_edge, pltpu.roll(row, cols - 1, 1))
            along_x = (0.5 * (k_mid + after[modes:modes + 1])) * (center - after[:modes]) + (
                0.5 * (k_mid + before[modes:modes + 1])
            ) * (center - before[:modes])
            along_y = (0.5 * (k_mid + to_right[modes:modes + 1])) * (center - to_right[:modes]) + (
                0.5 * (k_mid + to_left[modes:modes + 1])
            ) * (center - to_left[:modes])
            react = p_ref[pl.ds(i, 1), :] * center
            high, low = split(jnp.concatenate([center, along_x, along_y, react], 0))
            for t in range(tiles):
                at = pl.ds(pl.multiple_of((t * rows + i) * 128, 128), 128)
                m_ref[:columns, at] = high[:, t * 128:(t + 1) * 128]
                m_ref[columns:, at] = low[:, t * 128:(t + 1) * 128]
        for t in range(tiles):
            at = pl.ds(pl.multiple_of((t * rows + g * group) * 128, group * 128), group * 128)
            acc[...] += lax.dot_general(
                m_ref[:columns, at], m_ref[:, at], (((1,), (1,)), ((), ())), preferred_element_type=F32
            )
        return 0

    lax.fori_loop(0, rows // group, build, 0)
    cross = acc[:, columns:]
    total = (acc[:, :columns] + (cross + cross.T)) * (1.0 / (rows * cols * nx * ny))
    for j in range(ny):
        part[j] = total[j * share:(j + 1) * share]

    copies = [
        pltpu.make_async_remote_copy(
            src_ref=part.at[lax.rem(py + d, ny)], dst_ref=piece.at[py], send_sem=rs_send.at[d], recv_sem=rs_recv.at[d],
            device_id={"gy": lax.rem(py + d, ny)}, device_id_type=MESH,
        )
        for d in range(1, ny)
    ]
    for copy in copies:
        copy.start()
    piece[py] = part[py]
    for copy in copies:
        copy.wait()
    ring[px] = functools.reduce(jnp.add, [piece[j] for j in range(ny)])

    copies = [
        pltpu.make_async_remote_copy(
            src_ref=ring.at[px], dst_ref=ring.at[px], send_sem=all_send.at[d], recv_sem=all_recv.at[d],
            device_id={"gx": lax.rem(px + d, nx)}, device_id_type=MESH,
        )
        for d in range(1, nx)
    ]
    for copy in copies:
        copy.start()
    for copy in copies:
        copy.wait()
    full[py] = functools.reduce(jnp.add, [ring[j] for j in range(nx)])

    copies = [
        pltpu.make_async_remote_copy(
            src_ref=full.at[py], dst_ref=full.at[py], send_sem=ag_send.at[d], recv_sem=ag_recv.at[d],
            device_id={"gy": lax.rem(py + d, ny)}, device_id_type=MESH,
        )
        for d in range(1, ny)
    ]
    for copy in copies:
        copy.start()
    for copy in copies:
        copy.wait()
    for j in range(ny):
        g_ref[j * share:(j + 1) * share, :] = full[j]


def gram(fields, conduct, potential, nx, ny):
    modes, rows, cols = fields.shape
    columns = 4 * modes
    vmem = pl.BlockSpec(memory_space=pltpu.VMEM)
    dma = pltpu.SemaphoreType.DMA
    return pl.pallas_call(
        functools.partial(gram_kernel, nx, ny),
        out_shape=(
            jax.ShapeDtypeStruct((2 * columns, rows * cols), BF16),
            jax.ShapeDtypeStruct((columns, columns), F32),
        ),
        in_specs=[pl.BlockSpec(memory_space=pl.ANY), vmem, vmem],
        out_specs=(vmem, vmem),
        scratch_shapes=[
            pltpu.VMEM((cols // 128, modes * rows, 128), F32),
            dma((cols // 128,)),
            pltpu.VMEM((rows + 2, modes + 8, cols), F32),
            pltpu.VMEM((2, modes + 8, 128), F32),
            pltpu.VMEM((2, modes + 8, 128), F32),
            pltpu.VMEM((columns, 2 * columns), F32),
            pltpu.VMEM((ny, columns // ny, columns), F32),
            pltpu.VMEM((ny, columns // ny, columns), F32),
            pltpu.VMEM((nx, columns // ny, columns), F32),
            pltpu.VMEM((ny, columns // ny, columns), F32),
            dma((4,)), dma((4,)), dma((ny,)), dma((ny,)), dma((nx,)), dma((nx,)), dma((ny,)), dma((ny,)),
        ],
        compiler_params=pltpu.CompilerParams(
            collective_id=0, has_side_effects=True, vmem_limit_bytes=28 * 1024 * 1024
        ),
        name="gram",
    )(fields.reshape(modes * rows, cols), conduct, potential)


def apply_kernel(w_ref, m_ref, o_ref):
    columns, chunk, _ = o_ref.shape
    high, low = split(w_ref[...])
    weights = jnp.concatenate(
        [jnp.concatenate([high, high], 1), jnp.concatenate([low, jnp.zeros_like(low)], 1)], 0
    )
    flat = o_ref.reshape(columns * chunk, 128)
    for s in range(0, chunk, 2):
        both = jnp.dot(weights, m_ref[:, s * 128:(s + 2) * 128], preferred_element_type=F32)
        out = both[:columns] + both[columns:]
        for r in range(2):
            flat[pl.ds(s + r, columns, stride=chunk), :] = out[:, r * 128:(r + 1) * 128]


def apply(inverse, matrix, rows, cols):
    columns = inverse.shape[0]
    chunk = 16
    steps = rows // chunk
    return pl.pallas_call(
        apply_kernel,
        out_shape=jax.ShapeDtypeStruct((columns, rows, cols), F32),
        grid=(cols // 128, steps),
        in_specs=[
            pl.BlockSpec((columns, columns), lambda t, i: (0, 0)),
            pl.BlockSpec((2 * columns, chunk * 128), lambda t, i: (0, t * steps + i)),
        ],
        out_specs=pl.BlockSpec((columns, chunk, 128), lambda t, i: (0, i, t)),
        compiler_params=pltpu.CompilerParams(vmem_limit_bytes=16 * 1024 * 1024),
        name="apply",
    )(inverse, matrix)


def on_device(nx, ny, mode_fields, conductance, potential):
    modes, rows, cols = mode_fields.shape
    matrix, total = gram(mode_fields, conductance, potential, nx, ny)
    lower_tri = jnp.linalg.cholesky(total, symmetrize_input=False)
    inverse = jax.scipy.linalg.solve_triangular(lower_tri, jnp.eye(4 * modes, dtype=F32), lower=True)
    return apply(inverse, matrix, rows, cols), lower_tri.T


def solution(mesh):
    placed = (P(None, "gx", "gy"), P("gx", "gy"), P("gx", "gy"))
    return jax.shard_map(
        functools.partial(on_device, mesh.shape["gx"], mesh.shape["gy"]),
        mesh=mesh, in_specs=placed, out_specs=(P(None, "gx", "gy"), P()), check_vma=False,
    )
```

```python
import functools

import jax
import jax.numpy as jnp
from jax import lax
from jax.experimental import pallas as pl
from jax.experimental.pallas import tpu as pltpu
from jax.sharding import PartitionSpec as P

MESH = pl.DeviceIdType.MESH
F32 = jnp.float32
BF16 = jnp.bfloat16


def split(value):
    high = value.astype(BF16)
    return high, (value - high.astype(F32)).astype(BF16)


def gram_kernel(
    nx, ny, u_hbm, k_hbm, p_hbm, m_ref, g_ref,
    k_ref, p_ref, flat, load, wide, edge, halo, acc, part, piece, ring, full,
    halo_send, halo_recv, rs_send, rs_recv, all_send, all_recv, ag_send, ag_recv,
):
    rows, cols = k_hbm.shape
    modes = u_hbm.shape[0] // rows
    tiles = cols // 128
    columns = 4 * modes
    share = columns // ny
    px, py = lax.axis_index("gx"), lax.axis_index("gy")

    loads = [
        pltpu.make_async_copy(u_hbm.at[:, pl.ds(t * 128, 128)], flat.at[t], load.at[t]) for t in range(tiles)
    ]
    loads.append(pltpu.make_async_copy(k_hbm, k_ref, load.at[tiles]))
    loads.append(pltpu.make_async_copy(p_hbm, p_ref, load.at[tiles + 1]))
    for copy in loads:
        copy.start()
    barrier = pltpu.get_barrier_semaphore()
    for d in range(1, nx):
        pl.semaphore_signal(barrier, inc=1, device_id={"gx": lax.rem(px + d, nx)}, device_id_type=MESH)
    for d in range(1, ny):
        pl.semaphore_signal(barrier, inc=1, device_id={"gy": lax.rem(py + d, ny)}, device_id_type=MESH)

    lanes = lax.broadcasted_iota(jnp.int32, (modes + 8, 128), 1)

    def spread(i, carry):
        first, last = carry
        row = jnp.concatenate(
            [jnp.concatenate([flat[t, pl.ds(i, modes, stride=rows), :] for t in range(tiles)], 1),
             jnp.broadcast_to(k_ref[pl.ds(i, 1), :], (8, cols))], 0
        )
        wide[i + 1] = row
        first = jnp.where(lanes == i, pltpu.roll(row[:, :128], i, 1), first)
        last = jnp.where(lanes == i, pltpu.roll(row[:, cols - 128:], lax.rem(i + 1, 128), 1), last)
        return first, last

    for copy in loads:
        copy.wait()
    zero = jnp.zeros((modes + 8, 128), F32)
    first, last = lax.fori_loop(0, rows, spread, (zero, zero), unroll=4)
    edge[0] = first
    edge[1] = last

    pl.semaphore_wait(barrier, nx + ny - 2)
    right, left = lax.rem(py + 1, ny), lax.rem(py + ny - 1, ny)
    down, up = lax.rem(px + 1, nx), lax.rem(px + nx - 1, nx)
    moves = (
        (edge.at[1], halo.at[0], {"gy": right}),
        (edge.at[0], halo.at[1], {"gy": left}),
        (wide.at[rows], wide.at[0], {"gx": down}),
        (wide.at[1], wide.at[rows + 1], {"gx": up}),
    )
    copies = [
        pltpu.make_async_remote_copy(
            src_ref=src, dst_ref=dst, send_sem=halo_send.at[n], recv_sem=halo_recv.at[n],
            device_id=device, device_id_type=MESH,
        )
        for n, (src, dst, device) in enumerate(moves)
    ]
    for copy in copies:
        copy.start()
    for copy in copies:
        copy.wait()
    wide[0] = jnp.where(px > 0, wide[0], 0.0)
    wide[rows + 1] = jnp.where(px < nx - 1, wide[rows + 1], 0.0)
    halo[0] = jnp.where(py > 0, halo[0], 0.0)
    halo[1] = jnp.where(py < ny - 1, halo[1], 0.0)

    group = 4
    span = lax.broadcasted_iota(jnp.int32, (modes + 8, cols), 1)
    acc[...] = jnp.zeros_like(acc)

    def build(g, _):
        for s in range(group):
            i = g * group + s
            row = wide[i + 1]
            center, k_mid = row[:modes], row[modes:modes + 1]
            after, before = wide[i + 2], wide[i]
            pad = jnp.zeros((modes + 8, cols - 128), F32)
            left_edge = jnp.concatenate([pltpu.roll(halo[0], lax.rem(128 - i, 128), 1), pad], 1)
            right_edge = jnp.concatenate([pad, pltpu.roll(halo[1], 127 - i, 1)], 1)
            to_left = jnp.where(span == 0, left_edge, pltpu.roll(row, 1, 1))
            to_right = jnp.where(span == cols - 1, right_edge, pltpu.roll(row, cols - 1, 1))
            along_x = (0.5 * (k_mid + after[modes:modes + 1])) * (center - after[:modes]) + (
                0.5 * (k_mid + before[modes:modes + 1])
            ) * (center - before[:modes])
            along_y = (0.5 * (k_mid + to_right[modes:modes + 1])) * (center - to_right[:modes]) + (
                0.5 * (k_mid + to_left[modes:modes + 1])
            ) * (center - to_left[:modes])
            react = p_ref[pl.ds(i, 1), :] * center
            high, low = split(jnp.concatenate([center, along_x, along_y, react], 0))
            for t in range(tiles):
                at = pl.ds(pl.multiple_of((t * rows + i) * 128, 128), 128)
                m_ref[:columns, at] = high[:, t * 128:(t + 1) * 128]
                m_ref[columns:, at] = low[:, t * 128:(t + 1) * 128]
        for t in range(tiles):
            at = pl.ds(pl.multiple_of((t * rows + g * group) * 128, group * 128), group * 128)
            acc[...] += lax.dot_general(
                m_ref[:columns, at], m_ref[:, at], (((1,), (1,)), ((), ())), preferred_element_type=F32
            )
        return 0

    lax.fori_loop(0, rows // group, build, 0)
    cross = acc[:, columns:]
    total = (acc[:, :columns] + (cross + cross.T)) * (1.0 / (rows * cols * nx * ny))
    for j in range(ny):
        part[j] = total[j * share:(j + 1) * share]

    copies = [
        pltpu.make_async_remote_copy(
            src_ref=part.at[lax.rem(py + d, ny)], dst_ref=piece.at[py], send_sem=rs_send.at[d], recv_sem=rs_recv.at[d],
            device_id={"gy": lax.rem(py + d, ny)}, device_id_type=MESH,
        )
        for d in range(1, ny)
    ]
    for copy in copies:
        copy.start()
    piece[py] = part[py]
    for copy in copies:
        copy.wait()
    ring[px] = functools.reduce(jnp.add, [piece[j] for j in range(ny)])

    copies = [
        pltpu.make_async_remote_copy(
            src_ref=ring.at[px], dst_ref=ring.at[px], send_sem=all_send.at[d], recv_sem=all_recv.at[d],
            device_id={"gx": lax.rem(px + d, nx)}, device_id_type=MESH,
        )
        for d in range(1, nx)
    ]
    for copy in copies:
        copy.start()
    for copy in copies:
        copy.wait()
    full[py] = functools.reduce(jnp.add, [ring[j] for j in range(nx)])

    copies = [
        pltpu.make_async_remote_copy(
            src_ref=full.at[py], dst_ref=full.at[py], send_sem=ag_send.at[d], recv_sem=ag_recv.at[d],
            device_id={"gy": lax.rem(py + d, ny)}, device_id_type=MESH,
        )
        for d in range(1, ny)
    ]
    for copy in copies:
        copy.start()
    for copy in copies:
        copy.wait()
    for j in range(ny):
        g_ref[j * share:(j + 1) * share, :] = full[j]


def gram(fields, conduct, potential, nx, ny):
    modes, rows, cols = fields.shape
    columns = 4 * modes
    vmem = pl.BlockSpec(memory_space=pltpu.VMEM)
    dma = pltpu.SemaphoreType.DMA
    return pl.pallas_call(
        functools.partial(gram_kernel, nx, ny),
        out_shape=(
            jax.ShapeDtypeStruct((2 * columns, rows * cols), BF16),
            jax.ShapeDtypeStruct((columns, columns), F32),
        ),
        in_specs=[pl.BlockSpec(memory_space=pltpu.HBM)] * 3,
        out_specs=(vmem, vmem),
        scratch_shapes=[
            pltpu.VMEM((rows, cols), F32),
            pltpu.VMEM((rows, cols), F32),
            pltpu.VMEM((cols // 128, modes * rows, 128), F32),
            dma((cols // 128 + 2,)),
            pltpu.VMEM((rows + 2, modes + 8, cols), F32),
            pltpu.VMEM((2, modes + 8, 128), F32),
            pltpu.VMEM((2, modes + 8, 128), F32),
            pltpu.VMEM((columns, 2 * columns), F32),
            pltpu.VMEM((ny, columns // ny, columns), F32),
            pltpu.VMEM((ny, columns // ny, columns), F32),
            pltpu.VMEM((nx, columns // ny, columns), F32),
            pltpu.VMEM((ny, columns // ny, columns), F32),
            dma((4,)), dma((4,)), dma((ny,)), dma((ny,)), dma((nx,)), dma((nx,)), dma((ny,)), dma((ny,)),
        ],
        compiler_params=pltpu.CompilerParams(
            collective_id=0, has_side_effects=True, vmem_limit_bytes=66_900_000 - 4 * columns * rows * cols
        ),
        name="gram",
    )(fields.reshape(modes * rows, cols), conduct, potential)


def factor(g_ref, r_ref, w_ref):
    size = g_ref.shape[0]
    block = 8
    panels = size // block
    lane = lax.broadcasted_iota(jnp.int32, (block, size), 1)
    sub = lax.broadcasted_iota(jnp.int32, (block, size), 0)

    def stack(values):
        out = values[0]
        for j in range(1, block):
            out = jnp.where(sub == j, values[j], out)
        return out

    def row(value, j):
        return jnp.broadcast_to(value[j:j + 1], (block, size))

    def column(value, j):
        return jnp.broadcast_to(value[:, j:j + 1], (block, size))

    z = [g_ref[i * block:(i + 1) * block, :] for i in range(panels)]
    for p in range(panels):
        at = p * block
        diag = [column(z[p], at + j) for j in range(block)]
        a = [[row(diag[j], i) for j in range(i + 1)] for i in range(block)]
        low = [[None] * block for _ in range(block)]
        inv = [[None] * block for _ in range(block)]
        for j in range(block):
            root = lax.rsqrt(a[j][j])
            inv[j][j] = root
            for i in range(j + 1, block):
                low[i][j] = a[i][j] * root
            for i in range(j + 1, block):
                for k in range(j + 1, i + 1):
                    a[i][k] = a[i][k] - low[i][j] * low[k][j]
            for k in range(j):
                terms = [low[j][q] * inv[q][k] for q in range(k, j)]
                inv[j][k] = -root * functools.reduce(jnp.add, terms)
        inside = (lane >= at) & (lane < at + block)
        source = [row(z[p], k) for k in range(block)]
        swept = [jnp.where(inside, jnp.where(lane == at + k, 1.0, 0.0), source[k]) for k in range(block)]
        solved = [functools.reduce(jnp.add, [inv[j][k] * swept[k] for k in range(j + 1)]) for j in range(block)]
        upper = [functools.reduce(jnp.add, [inv[j][k] * source[k] for k in range(j + 1)]) for j in range(block)]
        r_ref[at:at + block, :] = jnp.where(lane >= at + sub, stack(upper), 0.0)
        w_ref[at:at + block, :] = jnp.where(lane <= at + sub, stack(solved), 0.0)
        if p + 1 < panels:
            both = [
                functools.reduce(jnp.add, [inv[j][k] * solved[j] for j in range(k, block)]) for k in range(block)
            ]
            for i in range(p + 1, panels):
                terms = [column(z[i], at + k) * both[k] for k in range(block)]
                z[i] = jnp.where(inside, 0.0, z[i]) - functools.reduce(jnp.add, terms)


def apply_kernel(g_ref, m_ref, o_ref, r_ref, w_ref, weights):
    columns, chunk, _ = o_ref.shape

    @pl.when((pl.program_id(0) == 0) & (pl.program_id(1) == 0))
    def _():
        factor(g_ref, r_ref, w_ref)
        high, low = split(w_ref[...])
        weights[:columns, :columns] = high
        weights[:columns, columns:] = high
        weights[columns:, :columns] = low
        weights[columns:, columns:] = jnp.zeros_like(low)

    flat = o_ref.reshape(columns * chunk, 128)
    for s in range(0, chunk, 2):
        both = jnp.dot(weights[...], m_ref[:, s * 128:(s + 2) * 128], preferred_element_type=F32)
        out = both[:columns] + both[columns:]
        for r in range(2):
            flat[pl.ds(s + r, columns, stride=chunk), :] = out[:, r * 128:(r + 1) * 128]


def apply(total, matrix, rows, cols):
    columns = total.shape[0]
    chunk = 16
    steps = rows // chunk
    square = pl.BlockSpec((columns, columns), lambda t, i: (0, 0))
    return pl.pallas_call(
        apply_kernel,
        out_shape=(
            jax.ShapeDtypeStruct((columns, rows, cols), F32),
            jax.ShapeDtypeStruct((columns, columns), F32),
        ),
        grid=(cols // 128, steps),
        in_specs=[square, pl.BlockSpec((2 * columns, chunk * 128), lambda t, i: (0, t * steps + i))],
        out_specs=(pl.BlockSpec((columns, chunk, 128), lambda t, i: (0, i, t)), square),
        scratch_shapes=[pltpu.VMEM((columns, columns), F32), pltpu.VMEM((2 * columns, 2 * columns), BF16)],
        compiler_params=pltpu.CompilerParams(vmem_limit_bytes=16 * 1024 * 1024),
        name="apply",
    )(total, matrix)


def on_device(nx, ny, mode_fields, conductance, potential):
    _, rows, cols = mode_fields.shape
    matrix, total = gram(mode_fields, conductance, potential, nx, ny)
    return apply(total, matrix, rows, cols)


def solution(mesh):
    placed = (P(None, "gx", "gy"), P("gx", "gy"), P("gx", "gy"))
    return jax.shard_map(
        functools.partial(on_device, mesh.shape["gx"], mesh.shape["gy"]),
        mesh=mesh, in_specs=placed, out_specs=(P(None, "gx", "gy"), P()), check_vma=False,
    )
```

```python
import functools

import jax
import jax.numpy as jnp
from jax import lax
from jax.experimental import pallas as pl
from jax.experimental.pallas import tpu as pltpu
from jax.sharding import PartitionSpec as P

MESH = pl.DeviceIdType.MESH
F32 = jnp.float32
BF16 = jnp.bfloat16


def split(value):
    high = value.astype(BF16)
    return high, (value - high.astype(F32)).astype(BF16)


def gram_kernel(
    nx, ny, u_hbm, k_hbm, p_hbm, m_ref, g_ref,
    k_ref, p_ref, flat, load, wide, edge, halo, acc, part, piece, ring, full,
    halo_send, halo_recv, rs_send, rs_recv, all_send, all_recv, ag_send, ag_recv,
):
    rows, cols = k_hbm.shape
    modes = u_hbm.shape[0]
    tiles = cols // 128
    columns = 4 * modes
    share = columns // ny
    px, py = lax.axis_index("gx"), lax.axis_index("gy")

    loads = [
        pltpu.make_async_copy(
            u_hbm.at[:, pl.ds(q * 8, 8), pl.ds(t * 128, 128)], flat.at[t, q], load.at[t * (rows // 8) + q]
        )
        for q in range(rows // 8)
        for t in range(tiles)
    ]
    loads.append(pltpu.make_async_copy(k_hbm, k_ref, load.at[tiles * rows // 8]))
    loads.append(pltpu.make_async_copy(p_hbm, p_ref, load.at[tiles * rows // 8 + 1]))
    for copy in loads:
        copy.start()
    barrier = pltpu.get_barrier_semaphore()
    for d in range(1, nx):
        pl.semaphore_signal(barrier, inc=1, device_id={"gx": lax.rem(px + d, nx)}, device_id_type=MESH)
    for d in range(1, ny):
        pl.semaphore_signal(barrier, inc=1, device_id={"gy": lax.rem(py + d, ny)}, device_id_type=MESH)

    lanes = lax.broadcasted_iota(jnp.int32, (modes + 8, 128), 1)

    blocks = flat.reshape(tiles, rows // 8, modes * 8, 128)

    def spread(q, carry):
        first, last = carry
        for s in range(8):
            i = q * 8 + s
            row = jnp.concatenate(
                [jnp.concatenate([blocks[t, q, pl.ds(s, modes, stride=8), :] for t in range(tiles)], 1),
                 jnp.broadcast_to(k_ref[pl.ds(i, 1), :], (8, cols))], 0
            )
            wide[i + 1] = row
            first = jnp.where(lanes == i, pltpu.roll(row[:, :128], i, 1), first)
            last = jnp.where(lanes == i, pltpu.roll(row[:, cols - 128:], lax.rem(i + 1, 128), 1), last)
        return first, last

    for copy in loads:
        copy.wait()
    zero = jnp.zeros((modes + 8, 128), F32)
    first, last = lax.fori_loop(0, rows // 8, spread, (zero, zero))
    edge[0] = first
    edge[1] = last

    pl.semaphore_wait(barrier, nx + ny - 2)
    right, left = lax.rem(py + 1, ny), lax.rem(py + ny - 1, ny)
    down, up = lax.rem(px + 1, nx), lax.rem(px + nx - 1, nx)
    moves = (
        (edge.at[1], halo.at[0], {"gy": right}),
        (edge.at[0], halo.at[1], {"gy": left}),
        (wide.at[rows], wide.at[0], {"gx": down}),
        (wide.at[1], wide.at[rows + 1], {"gx": up}),
    )
    copies = [
        pltpu.make_async_remote_copy(
            src_ref=src, dst_ref=dst, send_sem=halo_send.at[n], recv_sem=halo_recv.at[n],
            device_id=device, device_id_type=MESH,
        )
        for n, (src, dst, device) in enumerate(moves)
    ]
    for copy in copies:
        copy.start()
    for copy in copies:
        copy.wait()
    wide[0] = jnp.where(px > 0, wide[0], 0.0)
    wide[rows + 1] = jnp.where(px < nx - 1, wide[rows + 1], 0.0)
    halo[0] = jnp.where(py > 0, halo[0], 0.0)
    halo[1] = jnp.where(py < ny - 1, halo[1], 0.0)

    group = 4
    span = lax.broadcasted_iota(jnp.int32, (modes + 8, cols), 1)
    acc[...] = jnp.zeros_like(acc)

    def build(g, _):
        for s in range(group):
            i = g * group + s
            row = wide[i + 1]
            center, k_mid = row[:modes], row[modes:modes + 1]
            after, before = wide[i + 2], wide[i]
            pad = jnp.zeros((modes + 8, cols - 128), F32)
            left_edge = jnp.concatenate([pltpu.roll(halo[0], lax.rem(128 - i, 128), 1), pad], 1)
            right_edge = jnp.concatenate([pad, pltpu.roll(halo[1], 127 - i, 1)], 1)
            to_left = jnp.where(span == 0, left_edge, pltpu.roll(row, 1, 1))
            to_right = jnp.where(span == cols - 1, right_edge, pltpu.roll(row, cols - 1, 1))
            along_x = (0.5 * (k_mid + after[modes:modes + 1])) * (center - after[:modes]) + (
                0.5 * (k_mid + before[modes:modes + 1])
            ) * (center - before[:modes])
            along_y = (0.5 * (k_mid + to_right[modes:modes + 1])) * (center - to_right[:modes]) + (
                0.5 * (k_mid + to_left[modes:modes + 1])
            ) * (center - to_left[:modes])
            react = p_ref[pl.ds(i, 1), :] * center
            high, low = split(jnp.concatenate([center, along_x, along_y, react], 0))
            for t in range(tiles):
                at = pl.ds(pl.multiple_of((t * rows + i) * 128, 128), 128)
                m_ref[:columns, at] = high[:, t * 128:(t + 1) * 128]
                m_ref[columns:, at] = low[:, t * 128:(t + 1) * 128]
        for t in range(tiles):
            at = pl.ds(pl.multiple_of((t * rows + g * group) * 128, group * 128), group * 128)
            acc[...] += lax.dot_general(
                m_ref[:columns, at], m_ref[:, at], (((1,), (1,)), ((), ())), preferred_element_type=F32
            )
        return 0

    lax.fori_loop(0, rows // group, build, 0)
    cross = acc[:, columns:]
    total = (acc[:, :columns] + (cross + cross.T)) * (1.0 / (rows * cols * nx * ny))
    for j in range(ny):
        part[j] = total[j * share:(j + 1) * share]

    copies = [
        pltpu.make_async_remote_copy(
            src_ref=part.at[lax.rem(py + d, ny)], dst_ref=piece.at[py], send_sem=rs_send.at[d], recv_sem=rs_recv.at[d],
            device_id={"gy": lax.rem(py + d, ny)}, device_id_type=MESH,
        )
        for d in range(1, ny)
    ]
    for copy in copies:
        copy.start()
    piece[py] = part[py]
    for copy in copies:
        copy.wait()
    ring[px] = functools.reduce(jnp.add, [piece[j] for j in range(ny)])

    copies = [
        pltpu.make_async_remote_copy(
            src_ref=ring.at[px], dst_ref=ring.at[px], send_sem=all_send.at[d], recv_sem=all_recv.at[d],
            device_id={"gx": lax.rem(px + d, nx)}, device_id_type=MESH,
        )
        for d in range(1, nx)
    ]
    for copy in copies:
        copy.start()
    for copy in copies:
        copy.wait()
    full[py] = functools.reduce(jnp.add, [ring[j] for j in range(nx)])

    copies = [
        pltpu.make_async_remote_copy(
            src_ref=full.at[py], dst_ref=full.at[py], send_sem=ag_send.at[d], recv_sem=ag_recv.at[d],
            device_id={"gy": lax.rem(py + d, ny)}, device_id_type=MESH,
        )
        for d in range(1, ny)
    ]
    for copy in copies:
        copy.start()
    for copy in copies:
        copy.wait()
    for j in range(ny):
        g_ref[j * share:(j + 1) * share, :] = full[j]


def gram(fields, conduct, potential, nx, ny):
    modes, rows, cols = fields.shape
    columns = 4 * modes
    vmem = pl.BlockSpec(memory_space=pltpu.VMEM)
    dma = pltpu.SemaphoreType.DMA
    return pl.pallas_call(
        functools.partial(gram_kernel, nx, ny),
        out_shape=(
            pltpu.VMEM((2 * columns, rows * cols), BF16),
            pltpu.VMEM((columns, columns), F32),
        ),
        in_specs=[pl.BlockSpec(memory_space=pltpu.HBM)] * 3,
        out_specs=(vmem, vmem),
        scratch_shapes=[
            pltpu.VMEM((rows, cols), F32),
            pltpu.VMEM((rows, cols), F32),
            pltpu.VMEM((cols // 128, rows // 8, modes, 8, 128), F32),
            dma((cols // 128 * rows // 8 + 2,)),
            pltpu.VMEM((rows + 2, modes + 8, cols), F32),
            pltpu.VMEM((2, modes + 8, 128), F32),
            pltpu.VMEM((2, modes + 8, 128), F32),
            pltpu.VMEM((columns, 2 * columns), F32),
            pltpu.VMEM((ny, columns // ny, columns), F32),
            pltpu.VMEM((ny, columns // ny, columns), F32),
            pltpu.VMEM((nx, columns // ny, columns), F32),
            pltpu.VMEM((ny, columns // ny, columns), F32),
            dma((4,)), dma((4,)), dma((ny,)), dma((ny,)), dma((nx,)), dma((nx,)), dma((ny,)), dma((ny,)),
        ],
        compiler_params=pltpu.CompilerParams(
            collective_id=0, has_side_effects=True, vmem_limit_bytes=28 * 1024 * 1024
        ),
        name="gram",
    )(*(pltpu.with_memory_space_constraint(a, pltpu.HBM) for a in (fields, conduct, potential)))


def factor(g_ref, r_ref, w_ref):
    size = g_ref.shape[0]
    block = 8
    panels = size // block
    lane = lax.broadcasted_iota(jnp.int32, (block, size), 1)
    sub = lax.broadcasted_iota(jnp.int32, (block, size), 0)

    def stack(values):
        out = values[0]
        for j in range(1, block):
            out = jnp.where(sub == j, values[j], out)
        return out

    def row(value, j):
        return jnp.broadcast_to(value[j:j + 1], (block, size))

    def column(value, j):
        return jnp.broadcast_to(value[:, j:j + 1], (block, size))

    z = [g_ref[i * block:(i + 1) * block, :] for i in range(panels)]
    for p in range(panels):
        at = p * block
        diag = [column(z[p], at + j) for j in range(block)]
        a = [[row(diag[j], i) for j in range(i + 1)] for i in range(block)]
        low = [[None] * block for _ in range(block)]
        inv = [[None] * block for _ in range(block)]
        for j in range(block):
            root = lax.rsqrt(a[j][j])
            inv[j][j] = root
            for i in range(j + 1, block):
                low[i][j] = a[i][j] * root
            for i in range(j + 1, block):
                for k in range(j + 1, i + 1):
                    a[i][k] = a[i][k] - low[i][j] * low[k][j]
            for k in range(j):
                terms = [low[j][q] * inv[q][k] for q in range(k, j)]
                inv[j][k] = -root * functools.reduce(jnp.add, terms)
        inside = (lane >= at) & (lane < at + block)
        source = [row(z[p], k) for k in range(block)]
        swept = [jnp.where(inside, jnp.where(lane == at + k, 1.0, 0.0), source[k]) for k in range(block)]
        solved = [functools.reduce(jnp.add, [inv[j][k] * swept[k] for k in range(j + 1)]) for j in range(block)]
        upper = [functools.reduce(jnp.add, [inv[j][k] * source[k] for k in range(j + 1)]) for j in range(block)]
        r_ref[at:at + block, :] = jnp.where(lane >= at + sub, stack(upper), 0.0)
        w_ref[at:at + block, :] = jnp.where(lane <= at + sub, stack(solved), 0.0)
        if p + 1 < panels:
            both = [
                functools.reduce(jnp.add, [inv[j][k] * solved[j] for j in range(k, block)]) for k in range(block)
            ]
            for i in range(p + 1, panels):
                terms = [column(z[i], at + k) * both[k] for k in range(block)]
                z[i] = jnp.where(inside, 0.0, z[i]) - functools.reduce(jnp.add, terms)


def apply_kernel(g_ref, m_ref, o_ref, r_ref, w_ref, weights):
    columns, chunk, _ = o_ref.shape

    @pl.when((pl.program_id(0) == 0) & (pl.program_id(1) == 0))
    def _():
        factor(g_ref, r_ref, w_ref)
        high, low = split(w_ref[...])
        weights[:columns, :columns] = high
        weights[:columns, columns:] = high
        weights[columns:, :columns] = low
        weights[columns:, columns:] = jnp.zeros_like(low)

    flat = o_ref.reshape(columns * chunk, 128)
    for s in range(0, chunk, 2):
        both = jnp.dot(weights[...], m_ref[:, s * 128:(s + 2) * 128], preferred_element_type=F32)
        out = both[:columns] + both[columns:]
        for r in range(2):
            flat[pl.ds(s + r, columns, stride=chunk), :] = out[:, r * 128:(r + 1) * 128]


def apply(total, matrix, rows, cols):
    columns = total.shape[0]
    chunk = 8
    steps = rows // chunk
    square = pl.BlockSpec((columns, columns), lambda t, i: (0, 0))
    return pl.pallas_call(
        apply_kernel,
        out_shape=(
            jax.ShapeDtypeStruct((columns, rows, cols), F32),
            jax.ShapeDtypeStruct((columns, columns), F32),
        ),
        grid=(cols // 128, steps),
        in_specs=[square, pl.BlockSpec((2 * columns, chunk * 128), lambda t, i: (0, t * steps + i))],
        out_specs=(pl.BlockSpec((columns, chunk, 128), lambda t, i: (0, i, t)), square),
        scratch_shapes=[pltpu.VMEM((columns, columns), F32), pltpu.VMEM((2 * columns, 2 * columns), BF16)],
        compiler_params=pltpu.CompilerParams(vmem_limit_bytes=16 * 1024 * 1024),
        name="apply",
    )(total, matrix)


def on_device(nx, ny, mode_fields, conductance, potential):
    _, rows, cols = mode_fields.shape
    matrix, total = gram(mode_fields, conductance, potential, nx, ny)
    return apply(total, matrix, rows, cols)


def solution(mesh):
    placed = (P(None, "gx", "gy"), P("gx", "gy"), P("gx", "gy"))
    return jax.shard_map(
        functools.partial(on_device, mesh.shape["gx"], mesh.shape["gy"]),
        mesh=mesh, in_specs=placed, out_specs=(P(None, "gx", "gy"), P()), check_vma=False,
    )
```

```python
import functools

import jax
import jax.numpy as jnp
from jax import lax
from jax.experimental import pallas as pl
from jax.experimental.pallas import tpu as pltpu
from jax.sharding import PartitionSpec as P

MESH = pl.DeviceIdType.MESH
F32 = jnp.float32
BF16 = jnp.bfloat16


def split(value):
    high = value.astype(BF16)
    return high, (value - high.astype(F32)).astype(BF16)


def gram_kernel(
    nx, ny, u_hbm, k_hbm, p_hbm, m_ref, g_ref,
    k_ref, p_ref, flat, load, wide, edge, halo, acc, part, piece, ring, full,
    halo_send, halo_recv, rs_send, rs_recv, all_send, all_recv, ag_send, ag_recv,
):
    rows, cols = k_hbm.shape
    modes = u_hbm.shape[0]
    tiles = cols // 128
    columns = 4 * modes
    share = columns // ny
    px, py = lax.axis_index("gx"), lax.axis_index("gy")

    loads = [
        pltpu.make_async_copy(
            u_hbm.at[:, pl.ds(q * 8, 8), pl.ds(t * 128, 128)], flat.at[t, q], load.at[t * (rows // 8) + q]
        )
        for q in range(rows // 8)
        for t in range(tiles)
    ]
    loads.append(pltpu.make_async_copy(k_hbm, k_ref, load.at[tiles * rows // 8]))
    loads.append(pltpu.make_async_copy(p_hbm, p_ref, load.at[tiles * rows // 8 + 1]))
    for copy in loads:
        copy.start()
    barrier = pltpu.get_barrier_semaphore()
    for d in range(1, nx):
        pl.semaphore_signal(barrier, inc=1, device_id={"gx": lax.rem(px + d, nx)}, device_id_type=MESH)
    for d in range(1, ny):
        pl.semaphore_signal(barrier, inc=1, device_id={"gy": lax.rem(py + d, ny)}, device_id_type=MESH)

    lanes = lax.broadcasted_iota(jnp.int32, (modes + 8, 128), 1)

    blocks = flat.reshape(tiles, rows // 8, modes * 8, 128)

    def spread(q, carry):
        first, last = carry
        for s in range(8):
            i = q * 8 + s
            row = jnp.concatenate(
                [jnp.concatenate([blocks[t, q, pl.ds(s, modes, stride=8), :] for t in range(tiles)], 1),
                 jnp.broadcast_to(k_ref[pl.ds(i, 1), :], (8, cols))], 0
            )
            wide[i + 1] = row
            first = jnp.where(lanes == i, pltpu.roll(row[:, :128], i, 1), first)
            last = jnp.where(lanes == i, pltpu.roll(row[:, cols - 128:], lax.rem(i + 1, 128), 1), last)
        return first, last

    for copy in loads:
        copy.wait()
    zero = jnp.zeros((modes + 8, 128), F32)
    first, last = lax.fori_loop(0, rows // 8, spread, (zero, zero))
    edge[0] = first
    edge[1] = last

    pl.semaphore_wait(barrier, nx + ny - 2)
    right, left = lax.rem(py + 1, ny), lax.rem(py + ny - 1, ny)
    down, up = lax.rem(px + 1, nx), lax.rem(px + nx - 1, nx)
    moves = (
        (edge.at[1], halo.at[0], {"gy": right}),
        (edge.at[0], halo.at[1], {"gy": left}),
        (wide.at[rows], wide.at[0], {"gx": down}),
        (wide.at[1], wide.at[rows + 1], {"gx": up}),
    )
    copies = [
        pltpu.make_async_remote_copy(
            src_ref=src, dst_ref=dst, send_sem=halo_send.at[n], recv_sem=halo_recv.at[n],
            device_id=device, device_id_type=MESH,
        )
        for n, (src, dst, device) in enumerate(moves)
    ]
    for copy in copies:
        copy.start()
    for copy in copies:
        copy.wait()
    wide[0] = jnp.where(px > 0, wide[0], 0.0)
    wide[rows + 1] = jnp.where(px < nx - 1, wide[rows + 1], 0.0)
    halo[0] = jnp.where(py > 0, halo[0], 0.0)
    halo[1] = jnp.where(py < ny - 1, halo[1], 0.0)

    group = 4
    span = lax.broadcasted_iota(jnp.int32, (modes + 8, cols), 1)
    acc[...] = jnp.zeros_like(acc)

    def build(g, _):
        for s in range(group):
            i = g * group + s
            row = wide[i + 1]
            center, k_mid = row[:modes], row[modes:modes + 1]
            after, before = wide[i + 2], wide[i]
            pad = jnp.zeros((modes + 8, cols - 128), F32)
            left_edge = jnp.concatenate([pltpu.roll(halo[0], lax.rem(128 - i, 128), 1), pad], 1)
            right_edge = jnp.concatenate([pad, pltpu.roll(halo[1], 127 - i, 1)], 1)
            to_left = jnp.where(span == 0, left_edge, pltpu.roll(row, 1, 1))
            to_right = jnp.where(span == cols - 1, right_edge, pltpu.roll(row, cols - 1, 1))
            along_x = (0.5 * (k_mid + after[modes:modes + 1])) * (center - after[:modes]) + (
                0.5 * (k_mid + before[modes:modes + 1])
            ) * (center - before[:modes])
            along_y = (0.5 * (k_mid + to_right[modes:modes + 1])) * (center - to_right[:modes]) + (
                0.5 * (k_mid + to_left[modes:modes + 1])
            ) * (center - to_left[:modes])
            react = p_ref[pl.ds(i, 1), :] * center
            high, low = split(jnp.concatenate([center, along_x, along_y, react], 0))
            for t in range(tiles):
                at = pl.ds(pl.multiple_of((t * rows + i) * 128, 128), 128)
                m_ref[:columns, at] = high[:, t * 128:(t + 1) * 128]
                m_ref[columns:, at] = low[:, t * 128:(t + 1) * 128]
        for t in range(tiles):
            at = pl.ds(pl.multiple_of((t * rows + g * group) * 128, group * 128), group * 128)
            acc[...] += lax.dot_general(
                m_ref[:columns, at], m_ref[:, at], (((1,), (1,)), ((), ())), preferred_element_type=F32
            )
        return 0

    lax.fori_loop(0, rows // group, build, 0)
    cross = acc[:, columns:]
    total = (acc[:, :columns] + (cross + cross.T)) * (1.0 / (rows * cols * nx * ny))
    for j in range(ny):
        part[j] = total[j * share:(j + 1) * share]

    copies = [
        pltpu.make_async_remote_copy(
            src_ref=part.at[lax.rem(py + d, ny)], dst_ref=piece.at[py], send_sem=rs_send.at[d], recv_sem=rs_recv.at[d],
            device_id={"gy": lax.rem(py + d, ny)}, device_id_type=MESH,
        )
        for d in range(1, ny)
    ]
    for copy in copies:
        copy.start()
    piece[py] = part[py]
    for copy in copies:
        copy.wait()
    ring[px] = functools.reduce(jnp.add, [piece[j] for j in range(ny)])

    copies = [
        pltpu.make_async_remote_copy(
            src_ref=ring.at[px], dst_ref=ring.at[px], send_sem=all_send.at[d], recv_sem=all_recv.at[d],
            device_id={"gx": lax.rem(px + d, nx)}, device_id_type=MESH,
        )
        for d in range(1, nx)
    ]
    for copy in copies:
        copy.start()
    for copy in copies:
        copy.wait()
    full[py] = functools.reduce(jnp.add, [ring[j] for j in range(nx)])

    copies = [
        pltpu.make_async_remote_copy(
            src_ref=full.at[py], dst_ref=full.at[py], send_sem=ag_send.at[d], recv_sem=ag_recv.at[d],
            device_id={"gy": lax.rem(py + d, ny)}, device_id_type=MESH,
        )
        for d in range(1, ny)
    ]
    for copy in copies:
        copy.start()
    for copy in copies:
        copy.wait()
    for j in range(ny):
        g_ref[j * share:(j + 1) * share, :] = full[j]


def gram(fields, conduct, potential, nx, ny):
    modes, rows, cols = fields.shape
    columns = 4 * modes
    vmem = pl.BlockSpec(memory_space=pltpu.VMEM)
    dma = pltpu.SemaphoreType.DMA
    return pl.pallas_call(
        functools.partial(gram_kernel, nx, ny),
        out_shape=(
            pltpu.VMEM((2 * columns, rows * cols), BF16),
            pltpu.VMEM((columns, columns), F32),
        ),
        in_specs=[pl.BlockSpec(memory_space=pltpu.HBM)] * 3,
        out_specs=(vmem, vmem),
        scratch_shapes=[
            pltpu.VMEM((rows, cols), F32),
            pltpu.VMEM((rows, cols), F32),
            pltpu.VMEM((cols // 128, rows // 8, modes, 8, 128), F32),
            dma((cols // 128 * rows // 8 + 2,)),
            pltpu.VMEM((rows + 2, modes + 8, cols), F32),
            pltpu.VMEM((2, modes + 8, 128), F32),
            pltpu.VMEM((2, modes + 8, 128), F32),
            pltpu.VMEM((columns, 2 * columns), F32),
            pltpu.VMEM((ny, columns // ny, columns), F32),
            pltpu.VMEM((ny, columns // ny, columns), F32),
            pltpu.VMEM((nx, columns // ny, columns), F32),
            pltpu.VMEM((ny, columns // ny, columns), F32),
            dma((4,)), dma((4,)), dma((ny,)), dma((ny,)), dma((nx,)), dma((nx,)), dma((ny,)), dma((ny,)),
        ],
        compiler_params=pltpu.CompilerParams(
            collective_id=0, has_side_effects=True, vmem_limit_bytes=28 * 1024 * 1024
        ),
        name="gram",
    )(*(pltpu.with_memory_space_constraint(a, pltpu.HBM) for a in (fields, conduct, potential)))


def factor(g_ref, r_ref, w_ref):
    size = g_ref.shape[0]
    block = 8
    panels = size // block
    lane = lax.broadcasted_iota(jnp.int32, (block, size), 1)
    sub = lax.broadcasted_iota(jnp.int32, (block, size), 0)

    def stack(values):
        out = values[0]
        for j in range(1, block):
            out = jnp.where(sub == j, values[j], out)
        return out

    def row(value, j):
        return jnp.broadcast_to(value[j:j + 1], (block, size))

    def column(value, j):
        return jnp.broadcast_to(value[:, j:j + 1], (block, size))

    z = [g_ref[i * block:(i + 1) * block, :] for i in range(panels)]
    for p in range(panels):
        at = p * block
        diag = [column(z[p], at + j) for j in range(block)]
        a = [[row(diag[j], i) for j in range(i + 1)] for i in range(block)]
        low = [[None] * block for _ in range(block)]
        inv = [[None] * block for _ in range(block)]
        for j in range(block):
            root = lax.rsqrt(a[j][j])
            inv[j][j] = root
            for i in range(j + 1, block):
                low[i][j] = a[i][j] * root
            for i in range(j + 1, block):
                for k in range(j + 1, i + 1):
                    a[i][k] = a[i][k] - low[i][j] * low[k][j]
            for k in range(j):
                terms = [low[j][q] * inv[q][k] for q in range(k, j)]
                inv[j][k] = -root * functools.reduce(jnp.add, terms)
        inside = (lane >= at) & (lane < at + block)
        source = [row(z[p], k) for k in range(block)]
        swept = [jnp.where(inside, jnp.where(lane == at + k, 1.0, 0.0), source[k]) for k in range(block)]
        solved = [functools.reduce(jnp.add, [inv[j][k] * swept[k] for k in range(j + 1)]) for j in range(block)]
        upper = [functools.reduce(jnp.add, [inv[j][k] * source[k] for k in range(j + 1)]) for j in range(block)]
        r_ref[at:at + block, :] = jnp.where(lane >= at + sub, stack(upper), 0.0)
        w_ref[at:at + block, :] = jnp.where(lane <= at + sub, stack(solved), 0.0)
        if p + 1 < panels:
            both = [
                functools.reduce(jnp.add, [inv[j][k] * solved[j] for j in range(k, block)]) for k in range(block)
            ]
            for i in range(p + 1, panels):
                terms = [column(z[i], at + k) * both[k] for k in range(block)]
                z[i] = jnp.where(inside, 0.0, z[i]) - functools.reduce(jnp.add, terms)


def apply_kernel(g_ref, m_ref, o_hbm, r_ref, w_ref, weights, out, sent):
    parts, columns, chunk, _ = out.shape
    per = o_hbm.shape[1] // chunk
    factor(g_ref, r_ref, w_ref)
    high, low = split(w_ref[...])
    weights[:columns, :columns] = high
    weights[:columns, columns:] = high
    weights[columns:, :columns] = low
    weights[columns:, columns:] = jnp.zeros_like(low)
    flat = out.reshape(parts, columns * chunk, 128)

    def send(q):
        to = o_hbm.at[:, pl.ds(lax.rem(q, per) * chunk, chunk), pl.ds(pl.multiple_of(q // per * 128, 128), 128)]
        return pltpu.make_async_copy(out.at[q], to, sent.at[q])

    def step(q, _):
        for s in range(0, chunk, 2):
            at = pl.ds(pl.multiple_of((q * chunk + s) * 128, 256), 256)
            both = jnp.dot(weights[...], m_ref[:, at], preferred_element_type=F32)
            value = both[:columns] + both[columns:]
            for r in range(2):
                flat[q, pl.ds(s + r, columns, stride=chunk), :] = value[:, r * 128:(r + 1) * 128]
        send(q).start()
        return 0

    def finish(q, _):
        send(q).wait()
        return 0

    lax.fori_loop(0, parts, step, 0)
    lax.fori_loop(0, parts, finish, 0)


def apply(total, matrix, rows, cols):
    columns = total.shape[0]
    chunk = 8
    parts = (rows // chunk) * (cols // 128)
    vmem = pl.BlockSpec(memory_space=pltpu.VMEM)
    return pl.pallas_call(
        apply_kernel,
        out_shape=(
            jax.ShapeDtypeStruct((columns, rows, cols), F32),
            jax.ShapeDtypeStruct((columns, columns), F32),
        ),
        in_specs=[vmem, vmem],
        out_specs=(pl.BlockSpec(memory_space=pltpu.HBM), vmem),
        scratch_shapes=[
            pltpu.VMEM((columns, columns), F32),
            pltpu.VMEM((2 * columns, 2 * columns), BF16),
            pltpu.VMEM((parts, columns, chunk, 128), F32),
            pltpu.SemaphoreType.DMA((parts,)),
        ],
        compiler_params=pltpu.CompilerParams(vmem_limit_bytes=20 * 1024 * 1024),
        name="apply",
    )(total, pltpu.with_memory_space_constraint(matrix, pltpu.VMEM))


def on_device(nx, ny, mode_fields, conductance, potential):
    _, rows, cols = mode_fields.shape
    matrix, total = gram(mode_fields, conductance, potential, nx, ny)
    return apply(total, matrix, rows, cols)


def solution(mesh):
    placed = (P(None, "gx", "gy"), P("gx", "gy"), P("gx", "gy"))
    return jax.shard_map(
        functools.partial(on_device, mesh.shape["gx"], mesh.shape["gy"]),
        mesh=mesh, in_specs=placed, out_specs=(P(None, "gx", "gy"), P()), check_vma=False,
    )
```
